8 devices in a mesh: dp: 1 (over z), tp: 8 (over x, y, core).
Axes of the slice: x: 2, y: 2, z: 1, core: 2. Of those that a mesh axis runs over, the one named last changes fastest.
Arguments:
- x: bfloat16 [2048, 5376], P('dp')
- w_gate: bfloat16 [5376, 21504], P(None, 'tp')
- w_up: bfloat16 [5376, 21504], P(None, 'tp')
- w_down: bfloat16 [21504, 5376], P('tp')
Outputs:
- output: bfloat16 [2048, 5376], P('dp')
All inputs are finite; a program needn't handle non-finite values.
Results may differ from the reference program's by a relative error of at most 0.016.
Values are sent between devices in bfloat16 or wider.
A program may use at most 2 GiB of HBM per device.

```python
import jax
import jax.numpy as jnp

ROWS = 2048
D = 5376
FF = 21504


def setup_inputs(seed: int = 0, part: int = 0) -> dict:
    kx, kg, ku, kd = jax.random.split(jax.random.key(seed), 4)
    drawn = {
        "x": jax.random.normal(jax.random.fold_in(kx, part), (ROWS, D), jnp.float32),
        "w_gate": jax.random.normal(kg, (D, FF), jnp.float32) * D**-0.5,
        "w_up": jax.random.normal(ku, (D, FF), jnp.float32) * D**-0.5,
        "w_down": jax.random.normal(kd, (FF, D), jnp.float32) * FF**-0.5,
    }
    return {k: v.astype(jnp.bfloat16) for k, v in drawn.items()}


def reference(x, w_gate, w_up, w_down):
    gate = jnp.dot(x, w_gate, preferred_element_type=jnp.float32)
    up = jnp.dot(x, w_up, preferred_element_type=jnp.float32)
    hidden = (jax.nn.gelu(gate) * up).astype(jnp.bfloat16)
    return jnp.dot(hidden, w_down, preferred_element_type=jnp.float32).astype(jnp.bfloat16)
```

```python
import jax
import jax.numpy as jnp
from jax import lax
from jax.experimental import pallas as pl
from jax.experimental.pallas import tpu as pltpu
from jax.sharding import PartitionSpec as P

MESH = pl.DeviceIdType.MESH
ROWS, D, FF = 2048, 5376, 2688
GROUP = 512
HALF, QUARTER, SIXTH = GROUP // 2, GROUP // 8, GROUP // 16
GROUPS = ROWS // GROUP
T1 = 384
T2 = 768
TILES = FF // T1
PERIOD = 2 * TILES
OFFSETS = (2, 4, 6, 8, 10, 12)
S0, S1, S2, G1, G2, G3 = 0, 1, 3, 5, 7, 9


def kernel(x_hbm, wg, wu, wd, y, xbuf, wbuf, wdbuf, hid, acc, s0s, s0r, s1s, s1r, s2s, s2r, fin, xsem, wsem, wdsem, ssem, rsem, lsem):
    me = lax.axis_index("tp")
    cx, cy, core = me // 4, (me // 2) % 2, me % 2
    pn = me + 1 - 2 * core
    xn = me + 4 - 8 * cx
    yn = me + 2 - 4 * cy

    barrier = pltpu.get_barrier_semaphore()
    for n in (pn, xn, yn):
        pl.semaphore_signal(barrier, inc=1, device_id={"tp": n}, device_id_type=MESH)
    pl.semaphore_wait(barrier, 3)

    a = lambda i, j: i * QUARTER + j * SIXTH
    b = lambda j, i: HALF // 2 + j * QUARTER + i * SIXTH
    blocks = (a(cx, cy), a(cx, 1 - cy), a(1 - cx, cy), a(1 - cx, 1 - cy), b(cy, cx), b(cy, 1 - cx), b(1 - cy, cx), b(1 - cy, 1 - cx))

    def x_copies(g):
        out = []
        for h, c in enumerate((core, 1 - core)):
            for k, off in enumerate(blocks):
                row = pl.multiple_of(g * GROUP + c * HALF + off, SIXTH)
                i = h * len(blocks) + k
                out.append(pltpu.make_async_copy(x_hbm.at[pl.ds(row, SIXTH)], xbuf.at[pl.ds(i * SIXTH, SIXTH)], xsem.at[i]))
        return out

    def w_copies(j, slot):
        cols = pl.ds(pl.multiple_of(j * T1, T1), T1)
        return [
            pltpu.make_async_copy(wg.at[:, cols], wbuf.at[slot, :, pl.ds(0, T1)], wsem.at[slot, 0]),
            pltpu.make_async_copy(wu.at[:, cols], wbuf.at[slot, :, pl.ds(T1, T1)], wsem.at[slot, 1]),
        ]

    def columns(j):
        return pl.ds(pl.multiple_of(j * T2, T2), T2)

    def wd_copy(j, slot):
        return pltpu.make_async_copy(wd.at[:, columns(j)], wdbuf.at[slot], wdsem.at[slot])

    def remote(src, dst, sem, j, to):
        return pltpu.make_async_remote_copy(src_ref=src, dst_ref=dst, send_sem=ssem.at[sem, j], recv_sem=rsem.at[sem, j], device_id={"tp": to}, device_id_type=MESH)

    def part(g, off, rows, j):
        return y.at[pl.ds(pl.multiple_of(g * GROUP + core * HALF + off, SIXTH), rows), columns(j)]

    def copies(stage, g, j):
        if stage == S0:
            return [remote(s0s.at[j], s0r.at[j], S0, j, pn)]
        if stage == S1:
            return [remote(s1s.at[j, i], s1r.at[j, i], S1 + i, j, (xn, yn)[i]) for i in range(2)]
        if stage == S2:
            return [remote(s2s.at[j, i], s2r.at[j, i], S2 + i, j, (yn, xn)[i]) for i in range(2)]
        if stage == G1:
            return [remote(fin.at[j, i], part(g, blocks[4 * i], SIXTH, j), G1 + i, j, (yn, xn)[i]) for i in range(2)]
        if stage == G2:
            offs = (cx * QUARTER, HALF // 2 + cy * QUARTER)
            return [remote(part(g, offs[i], QUARTER, j), part(g, offs[i], QUARTER, j), G2 + i, j, (xn, yn)[i]) for i in range(2)]
        return [remote(part(g, 0, HALF, j), part(g, 0, HALF, j), G3, j, pn)]

    def own(g, j):
        return [pltpu.make_async_copy(fin.at[j, i], part(g, blocks[4 * i], SIXTH, j), lsem.at[i, j]) for i in range(2)]

    def start(cs):
        for c in cs:
            c.start()

    def arrive(cs):
        for c in cs:
            c.wait_recv()

    f32, bf16 = jnp.float32, jnp.bfloat16
    Q, H = QUARTER, HALF // 2

    def stage1(g, j):
        arrive(copies(S0, g, j))
        for i in range(2):
            keep, send = pl.ds(i * H, Q), pl.ds(i * H + Q, Q)
            s1s[j, i] = (acc[j, send] + s0r[j, send].astype(f32)).astype(bf16)
            acc[j, keep] = acc[j, keep] + s0r[j, keep].astype(f32)
        start(copies(S1, g, j))

    def stage2(g, j):
        arrive(copies(S1, g, j))
        for i in range(2):
            keep, send = pl.ds(i * H, SIXTH), pl.ds(i * H + SIXTH, SIXTH)
            s2s[j, i] = (acc[j, send] + s1r[j, i, SIXTH:].astype(f32)).astype(bf16)
            acc[j, keep] = acc[j, keep] + s1r[j, i, :SIXTH].astype(f32)
        start(copies(S2, g, j))

    def stage3(g, j):
        arrive(copies(S2, g, j))
        for i in range(2):
            fin[j, i] = (acc[j, pl.ds(i * H, SIXTH)] + s2r[j, i].astype(f32)).astype(bf16)
        start(copies(G1, g, j))
        start(own(g, j))

    def stage4(g, j):
        for c in own(g, j):
            c.wait()
        arrive(copies(G1, g, j))
        start(copies(G2, g, j))

    def stage5(g, j):
        arrive(copies(G2, g, j))
        start(copies(G3, g, j))

    def stage6(g, j):
        arrive(copies(G3, g, j))
        for stage in (S0, S1, S2, G1, G2, G3):
            for c in copies(stage, g, j):
                c.wait_send()

    def service(tick):
        for fn, off in zip((stage1, stage2, stage3, stage4, stage5, stage6), OFFSETS):
            w = tick - TILES - off
            pos = lax.max(w, 0)
            g, j = pos // PERIOD, pos % PERIOD

            @pl.when((w >= 0) & (j < TILES) & (g < GROUPS))
            def _():
                fn(g, j)

    start(x_copies(0))
    start(w_copies(0, 0))
    wd_copy(0, 0).start()

    def group(g, _):
        for c in x_copies(g):
            c.wait()

        def first(j, _):
            n = g * TILES + j
            slot = n % 2

            @pl.when(n + 1 < GROUPS * TILES)
            def _():
                start(w_copies((j + 1) % TILES, 1 - slot))

            service(g * PERIOD + j)
            for c in w_copies(j, slot):
                c.wait()
            r = jnp.dot(xbuf[...], wbuf[slot], preferred_element_type=f32)
            hid[:, pl.ds(pl.multiple_of(j * T1, T1), T1)] = (jax.nn.gelu(r[:, :T1]) * r[:, T1:]).astype(bf16)
            return 0

        lax.fori_loop(0, TILES, first, 0)

        @pl.when(g + 1 < GROUPS)
        def _():
            start(x_copies(g + 1))

        def second(j, _):
            n = g * TILES + j
            slot = n % 2

            @pl.when(n + 1 < GROUPS * TILES)
            def _():
                wd_copy((j + 1) % TILES, 1 - slot).start()

            service(g * PERIOD + TILES + j)
            wd_copy(j, slot).wait()
            r = jnp.dot(hid[...], wdbuf[slot], preferred_element_type=f32)
            acc[j] = r[:HALF]
            s0s[j] = r[HALF:].astype(bf16)
            start(copies(S0, g, j))
            return 0

        lax.fori_loop(0, TILES, second, 0)
        return 0

    lax.fori_loop(0, GROUPS, group, 0)

    def drain(i, _):
        service(GROUPS * PERIOD + i)
        return 0

    lax.fori_loop(0, OFFSETS[-1], drain, 0)


def solution(mesh):
    bf16, f32 = jnp.bfloat16, jnp.float32

    def step(x, w_gate, w_up, w_down):
        return pl.pallas_call(
            kernel,
            out_shape=jax.ShapeDtypeStruct((ROWS, D), bf16),
            in_specs=[pl.BlockSpec(memory_space=pl.ANY)] * 4,
            out_specs=pl.BlockSpec(memory_space=pl.ANY),
            scratch_shapes=[
                pltpu.VMEM((GROUP, D), bf16),
                pltpu.VMEM((2, D, 2 * T1), bf16),
                pltpu.VMEM((2, FF, T2), bf16),
                pltpu.VMEM((GROUP, FF), bf16),
                pltpu.VMEM((TILES, HALF, T2), f32),
                pltpu.VMEM((TILES, HALF, T2), bf16),
                pltpu.VMEM((TILES, HALF, T2), bf16),
                pltpu.VMEM((TILES, 2, QUARTER, T2), bf16),
                pltpu.VMEM((TILES, 2, QUARTER, T2), bf16),
                pltpu.VMEM((TILES, 2, SIXTH, T2), bf16),
                pltpu.VMEM((TILES, 2, SIXTH, T2), bf16),
                pltpu.VMEM((TILES, 2, SIXTH, T2), bf16),
                pltpu.SemaphoreType.DMA((16,)),
                pltpu.SemaphoreType.DMA((2, 2)),
                pltpu.SemaphoreType.DMA((2,)),
                pltpu.SemaphoreType.DMA((10, TILES)),
                pltpu.SemaphoreType.DMA((10, TILES)),
                pltpu.SemaphoreType.DMA((2, TILES)),
            ],
            compiler_params=pltpu.CompilerParams(collective_id=0, has_side_effects=True, vmem_limit_bytes=67043328),
            cost_estimate=pl.CostEstimate(flops=6 * ROWS * D * FF, bytes_accessed=400 * 2**20, transcendentals=ROWS * FF),
        )(x, w_gate, w_up, w_down)

    return jax.shard_map(
        step,
        mesh=mesh,
        in_specs=(P("dp", None), P(None, "tp"), P(None, "tp"), P("tp", None)),
        out_specs=P("dp", None),
        check_vma=False,
    )
```

```python
import math

import jax
import jax.numpy as jnp
from jax import lax
from jax.experimental import pallas as pl
from jax.experimental.pallas import tpu as pltpu
from jax.sharding import PartitionSpec as P

MESH = pl.DeviceIdType.MESH
ROWS, D, FF = 2048, 5376, 2688
GROUP = 512
HALF, QUARTER, SIXTH = GROUP // 2, GROUP // 8, GROUP // 16
GROUPS = ROWS // GROUP
T1 = 384
T2 = 768
TILES = FF // T1
PERIOD = 2 * TILES
OFFSETS = (2, 4, 6, 8, 10, 12)
PIECES = 4
S0, S1, S2, G1, G2, G3 = 0, 1, 3, 5, 7, 9


def gelu(v):
    c = (2 / math.pi) ** 0.5
    return v * (0.5 + 0.5 * jnp.tanh(v * (c + (c * 0.044715) * (v * v))))


def kernel(x_hbm, wg, wu, wd, y, whole, xbuf, wdbuf, hid, acc, s1s, s1r, s2s, s2r, fin, xsem, wsem, wdsem, ssem, rsem, lsem, vsem):
    def wrows(slot):
        return pl.ds(pl.multiple_of(slot * D, 128), D)

    def srows(j, first=0, rows=HALF):
        return pl.ds(pl.multiple_of(2 * D + j * HALF + first, QUARTER), rows)

    def rrows(j, first=0, rows=HALF):
        return pl.ds(pl.multiple_of(2 * D + TILES * HALF + j * HALF + first, QUARTER), rows)

    me = lax.axis_index("tp")
    cx, cy, core = me // 4, (me // 2) % 2, me % 2
    pn = me + 1 - 2 * core
    xn = me + 4 - 8 * cx
    yn = me + 2 - 4 * cy

    barrier = pltpu.get_barrier_semaphore()
    for n in (pn, xn, yn):
        pl.semaphore_signal(barrier, inc=1, device_id={"tp": n}, device_id_type=MESH)
    pl.semaphore_wait(barrier, 3)

    a = lambda i, j: i * QUARTER + j * SIXTH
    b = lambda j, i: HALF // 2 + j * QUARTER + i * SIXTH
    blocks = (a(cx, cy), a(cx, 1 - cy), a(1 - cx, cy), a(1 - cx, 1 - cy), b(cy, cx), b(cy, 1 - cx), b(1 - cy, cx), b(1 - cy, 1 - cx))

    def x_copies(g):
        out = []
        for h, c in enumerate((core, 1 - core)):
            for k, off in enumerate(blocks):
                row = pl.multiple_of(g * GROUP + c * HALF + off, SIXTH)
                i = h * len(blocks) + k
                out.append(pltpu.make_async_copy(x_hbm.at[pl.ds(row, SIXTH)], xbuf.at[pl.ds(i * SIXTH, SIXTH)], xsem.at[i]))
        return out

    def w_copies(j, slot):
        cols = pl.ds(pl.multiple_of(j * T1, T1), T1)
        return [
            pltpu.make_async_copy(wg.at[:, cols], whole.at[wrows(slot), pl.ds(0, T1)], wsem.at[slot, 0]),
            pltpu.make_async_copy(wu.at[:, cols], whole.at[wrows(slot), pl.ds(T1, T1)], wsem.at[slot, 1]),
        ]

    def columns(j):
        return pl.ds(pl.multiple_of(j * T2, T2), T2)

    def wd_copy(j, slot):
        return pltpu.make_async_copy(wd.at[:, columns(j)], wdbuf.at[slot], wdsem.at[slot])

    def remote(src, dst, sem, j, to):
        return pltpu.make_async_remote_copy(src_ref=src, dst_ref=dst, send_sem=ssem.at[sem, j], recv_sem=rsem.at[sem, j], device_id={"tp": to}, device_id_type=MESH)

    def part(g, off, rows, j):
        return y.at[pl.ds(pl.multiple_of(g * GROUP + core * HALF + off, SIXTH), rows), columns(j)]

    def copies(stage, g, j):
        if stage == S0:
            return [remote(whole.at[srows(j)], whole.at[rrows(j)], S0, j, pn)]
        if stage == S1:
            return [remote(s1s.at[j, i], s1r.at[j, i], S1 + i, j, (xn, yn)[i]) for i in range(2)]
        if stage == S2:
            return [remote(s2s.at[j, i], s2r.at[j, i], S2 + i, j, (yn, xn)[i]) for i in range(2)]
        if stage == G1:
            return [remote(fin.at[j, i], part(g, blocks[4 * i], SIXTH, j), G1 + i, j, (yn, xn)[i]) for i in range(2)]
        if stage == G2:
            offs = (cx * QUARTER, HALF // 2 + cy * QUARTER)
            return [remote(part(g, offs[i], QUARTER, j), part(g, offs[i], QUARTER, j), G2 + i, j, (xn, yn)[i]) for i in range(2)]
        return [remote(part(g, 0, HALF, j), part(g, 0, HALF, j), G3, j, pn)]

    def own(g, j):
        return [pltpu.make_async_copy(fin.at[j, i], part(g, blocks[4 * i], SIXTH, j), lsem.at[i, j]) for i in range(2)]

    def start(cs):
        for c in cs:
            c.start()

    def arrive(cs):
        for c in cs:
            c.wait_recv()

    f32, bf16 = jnp.float32, jnp.bfloat16
    Q, H = QUARTER, HALF // 2

    def stage1(g, j):
        arrive(copies(S0, g, j))
        for i in range(2):
            keep, send = pl.ds(i * H, Q), pl.ds(i * H + Q, Q)
            s1s[j, i] = (acc[j, send] + whole[rrows(j, i * H + Q, Q), :].astype(f32)).astype(bf16)
            acc[j, keep] = acc[j, keep] + whole[rrows(j, i * H, Q), :].astype(f32)
        start(copies(S1, g, j))

    def stage2(g, j):
        arrive(copies(S1, g, j))
        for c in copies(S0, g, j):
            c.wait_send()
        for i in range(2):
            keep, send = pl.ds(i * H, SIXTH), pl.ds(i * H + SIXTH, SIXTH)
            s2s[j, i] = (acc[j, send] + s1r[j, i, SIXTH:].astype(f32)).astype(bf16)
            acc[j, keep] = acc[j, keep] + s1r[j, i, :SIXTH].astype(f32)
        start(copies(S2, g, j))

    def stage3(g, j):
        arrive(copies(S2, g, j))
        for i in range(2):
            fin[j, i] = (acc[j, pl.ds(i * H, SIXTH)] + s2r[j, i].astype(f32)).astype(bf16)
        start(copies(G1, g, j))
        start(own(g, j))

    def stage4(g, j):
        for c in own(g, j):
            c.wait()
        arrive(copies(G1, g, j))
        start(copies(G2, g, j))

    def stage5(g, j):
        arrive(copies(G2, g, j))
        start(copies(G3, g, j))

    def stage6(g, j):
        arrive(copies(G3, g, j))
        for stage in (S1, S2, G1, G2, G3):
            for c in copies(stage, g, j):
                c.wait_send()

    def service(tick):
        for fn, off in zip((stage1, stage2, stage3, stage4, stage5, stage6), OFFSETS):
            w = tick - TILES - off
            pos = lax.max(w, 0)
            g, j = pos // PERIOD, pos % PERIOD

            @pl.when((w >= 0) & (j < TILES) & (g < GROUPS))
            def _():
                fn(g, j)

    start(x_copies(0))
    start(w_copies(0, 0))
    wd_copy(0, 0).start()

    def group(g, _):
        for c in x_copies(g):
            c.wait()

        def first(j, _):
            n = g * TILES + j
            slot = n % 2

            @pl.when(n + 1 < GROUPS * TILES)
            def _():
                start(w_copies((j + 1) % TILES, 1 - slot))

            service(g * PERIOD + j)
            for c in w_copies(j, slot):
                c.wait()
            r = jnp.dot(xbuf[...], whole[wrows(slot), :], preferred_element_type=f32)
            hid[:, pl.ds(pl.multiple_of(j * T1, T1), T1)] = (gelu(r[:, :T1]) * r[:, T1:]).astype(bf16)
            return 0

        lax.fori_loop(0, TILES, first, 0)

        @pl.when(g + 1 < GROUPS)
        def _():
            start(x_copies(g + 1))

        def second(j, _):
            n = g * TILES + j
            slot = n % 2

            @pl.when(n + 1 < GROUPS * TILES)
            def _():
                wd_copy((j + 1) % TILES, 1 - slot).start()

            service(g * PERIOD + TILES + j)
            wd_copy(j, slot).wait()
            r = jnp.dot(hid[...], wdbuf[slot], preferred_element_type=f32)
            acc[j] = r[:HALF]
            whole[srows(j), :] = r[HALF:].astype(bf16)
            start(copies(S0, g, j))
            return 0

        lax.fori_loop(0, TILES, second, 0)
        return 0

    lax.fori_loop(0, GROUPS, group, 0)

    def settle(j, first, rows, sem):
        at = pl.ds(pl.multiple_of(j * ROWS + first, GROUP), rows)
        return pltpu.make_async_copy(y.at[pl.ds(first, rows), columns(j)], whole.at[at], vsem.at[sem, j])

    last, full = ROWS - GROUP, 2 * D // ROWS
    for i in range(OFFSETS[-1]):
        service(GROUPS * PERIOD + i)
        if i == 0:
            for j in range(full):
                settle(j, 0, last, 0).start()
        if i == OFFSETS[1]:
            for j in range(full, TILES):
                settle(j, 0, last, 0).start()
        j = i + TILES - OFFSETS[-1]
        if j >= 0:
            settle(j, last, GROUP, 1).start()
    for j in range(TILES):
        settle(j, 0, last, 0).wait()
        settle(j, last, GROUP, 1).wait()


def copy_kernel(whole, out, sem):
    rows = ROWS // PIECES
    cs = [
        pltpu.make_async_copy(whole.at[pl.ds(j * ROWS + i * rows, rows)], out.at[pl.ds(i * rows, rows), pl.ds(j * T2, T2)], sem.at[j, i])
        for i in range(PIECES)
        for j in range(TILES)
    ]
    for c in cs:
        c.start()
    for c in cs:
        c.wait()


def solution(mesh):
    bf16, f32 = jnp.bfloat16, jnp.float32

    def step(x, w_gate, w_up, w_down):
        _, whole = pl.pallas_call(
            kernel,
            out_shape=(jax.ShapeDtypeStruct((ROWS, D), bf16), pltpu.VMEM((TILES * ROWS, T2), bf16)),
            in_specs=[pl.BlockSpec(memory_space=pl.ANY)] * 4,
            out_specs=(pl.BlockSpec(memory_space=pl.ANY), pl.BlockSpec(memory_space=pltpu.VMEM)),
            scratch_shapes=[
                pltpu.VMEM((GROUP, D), bf16),
                pltpu.VMEM((2, FF, T2), bf16),
                pltpu.VMEM((GROUP, FF), bf16),
                pltpu.VMEM((TILES, HALF, T2), f32),
                pltpu.VMEM((TILES, 2, QUARTER, T2), bf16),
                pltpu.VMEM((TILES, 2, QUARTER, T2), bf16),
                pltpu.VMEM((TILES, 2, SIXTH, T2), bf16),
                pltpu.VMEM((TILES, 2, SIXTH, T2), bf16),
                pltpu.VMEM((TILES, 2, SIXTH, T2), bf16),
                pltpu.SemaphoreType.DMA((16,)),
                pltpu.SemaphoreType.DMA((2, 2)),
                pltpu.SemaphoreType.DMA((2,)),
                pltpu.SemaphoreType.DMA((10, TILES)),
                pltpu.SemaphoreType.DMA((10, TILES)),
                pltpu.SemaphoreType.DMA((2, TILES)),
                pltpu.SemaphoreType.DMA((2, TILES)),
            ],
            compiler_params=pltpu.CompilerParams(collective_id=0, has_side_effects=True, vmem_limit_bytes=42 * 2**20),
            cost_estimate=pl.CostEstimate(flops=6 * ROWS * D * FF, bytes_accessed=400 * 2**20, transcendentals=ROWS * FF),
        )(x, w_gate, w_up, w_down)
        return pl.pallas_call(
            copy_kernel,
            out_shape=jax.ShapeDtypeStruct((ROWS, D), bf16),
            in_specs=[pl.BlockSpec(memory_space=pltpu.VMEM)],
            out_specs=pl.BlockSpec(memory_space=pl.ANY),
            scratch_shapes=[pltpu.SemaphoreType.DMA((TILES, PIECES))],
            compiler_params=pltpu.CompilerParams(vmem_limit_bytes=4 * 2**20),
            cost_estimate=pl.CostEstimate(flops=0, bytes_accessed=2 * ROWS * D, transcendentals=0),
        )(whole)

    return jax.shard_map(
        step,
        mesh=mesh,
        in_specs=(P("dp", None), P(None, "tp"), P(None, "tp"), P("tp", None)),
        out_specs=P("dp", None),
        check_vma=False,
    )
```

```python
import math

import jax
import jax.numpy as jnp
from jax import lax
from jax.experimental import pallas as pl
from jax.experimental.pallas import tpu as pltpu
from jax.sharding import PartitionSpec as P

MESH = pl.DeviceIdType.MESH
ROWS, D, FF = 2048, 5376, 2688
GROUP = 512
HALF, QUARTER, SIXTH = GROUP // 2, GROUP // 8, GROUP // 16
GROUPS = ROWS // GROUP
T1 = 384
T2 = 768
TILES = FF // T1
PERIOD = 2 * TILES
OFFSETS = (2, 5, 7, 9, 12, 14)
PIECES = 4
S0, S1, S2, G1, G2, G3 = 0, 1, 3, 5, 7, 9


def gelu(v):
    c = (2 / math.pi) ** 0.5
    return v * (0.5 + 0.5 * jnp.tanh(v * (c + (c * 0.044715) * (v * v))))


def kernel(x_hbm, wg, wu, wd, y, whole, xbuf, wdbuf, hid, acc, s1s, s1r, s2s, s2r, fin, xsem, wsem, wdsem, ssem, rsem, lsem, vsem):
    def wrows(slot):
        return pl.ds(pl.multiple_of(slot * D, 128), D)

    def srows(j, first=0, rows=HALF):
        return pl.ds(pl.multiple_of(2 * D + j * HALF + first, QUARTER), rows)

    def rrows(j, first=0, rows=HALF):
        return pl.ds(pl.multiple_of(2 * D + TILES * HALF + j * HALF + first, QUARTER), rows)

    me = lax.axis_index("tp")
    cx, cy, core = me // 4, (me // 2) % 2, me % 2
    pn = me + 1 - 2 * core
    xn = me + 4 - 8 * cx
    yn = me + 2 - 4 * cy

    a = lambda i, j: i * QUARTER + j * SIXTH
    b = lambda j, i: HALF // 2 + j * QUARTER + i * SIXTH
    blocks = (a(cx, cy), a(cx, 1 - cy), a(1 - cx, cy), a(1 - cx, 1 - cy), b(cy, cx), b(cy, 1 - cx), b(1 - cy, cx), b(1 - cy, 1 - cx))

    def x_copies(g):
        out = []
        for h, c in enumerate((core, 1 - core)):
            for k, off in enumerate(blocks):
                row = pl.multiple_of(g * GROUP + c * HALF + off, SIXTH)
                i = h * len(blocks) + k
                out.append(pltpu.make_async_copy(x_hbm.at[pl.ds(row, SIXTH)], xbuf.at[pl.ds(i * SIXTH, SIXTH)], xsem.at[i]))
        return out

    def w_copies(j, slot):
        cols = pl.ds(pl.multiple_of(j * T1, T1), T1)
        return [
            pltpu.make_async_copy(wg.at[:, cols], whole.at[wrows(slot), pl.ds(0, T1)], wsem.at[slot, 0]),
            pltpu.make_async_copy(wu.at[:, cols], whole.at[wrows(slot), pl.ds(T1, T1)], wsem.at[slot, 1]),
        ]

    def columns(j):
        return pl.ds(pl.multiple_of(j * T2, T2), T2)

    def wd_copy(j, slot):
        return pltpu.make_async_copy(wd.at[:, columns(j)], wdbuf.at[slot], wdsem.at[slot])

    def remote(src, dst, sem, j, to):
        return pltpu.make_async_remote_copy(src_ref=src, dst_ref=dst, send_sem=ssem.at[sem, j], recv_sem=rsem.at[sem, j], device_id={"tp": to}, device_id_type=MESH)

    def part(g, off, rows, j):
        return y.at[pl.ds(pl.multiple_of(g * GROUP + core * HALF + off, SIXTH), rows), columns(j)]

    def copies(stage, g, j):
        if stage == S0:
            return [remote(whole.at[srows(j)], whole.at[rrows(j)], S0, j, pn)]
        if stage == S1:
            return [remote(s1s.at[j, i], s1r.at[j, i], S1 + i, j, (xn, yn)[i]) for i in range(2)]
        if stage == S2:
            return [remote(s2s.at[j, i], s2r.at[j, i], S2 + i, j, (yn, xn)[i]) for i in range(2)]
        if stage == G1:
            return [remote(fin.at[j, i], part(g, blocks[4 * i], SIXTH, j), G1 + i, j, (yn, xn)[i]) for i in range(2)]
        if stage == G2:
            offs = (cx * QUARTER, HALF // 2 + cy * QUARTER)
            return [remote(part(g, offs[i], QUARTER, j), part(g, offs[i], QUARTER, j), G2 + i, j, (xn, yn)[i]) for i in range(2)]
        return [remote(part(g, 0, HALF, j), part(g, 0, HALF, j), G3, j, pn)]

    def own(g, j):
        return [pltpu.make_async_copy(fin.at[j, i], part(g, blocks[4 * i], SIXTH, j), lsem.at[i, j]) for i in range(2)]

    def start(cs):
        for c in cs:
            c.start()

    def arrive(cs):
        for c in cs:
            c.wait_recv()

    f32, bf16 = jnp.float32, jnp.bfloat16
    Q, H = QUARTER, HALF // 2

    def sent(stage, g, j):
        for c in copies(stage, g, j):
            c.wait_send()

    def stage1(g, j):
        arrive(copies(S0, g, j))
        for i in range(2):
            keep, send = pl.ds(i * H, Q), pl.ds(i * H + Q, Q)
            s1s[j, i] = (acc[j, send] + whole[rrows(j, i * H + Q, Q), :].astype(f32)).astype(bf16)
            acc[j, keep] = acc[j, keep] + whole[rrows(j, i * H, Q), :].astype(f32)
        start(copies(S1, g, j))

    def stage2(g, j):
        arrive(copies(S1, g, j))
        sent(S0, g, j)
        for i in range(2):
            keep, send = pl.ds(i * H, SIXTH), pl.ds(i * H + SIXTH, SIXTH)
            s2s[j, i] = (acc[j, send] + s1r[j, i, SIXTH:].astype(f32)).astype(bf16)
            acc[j, keep] = acc[j, keep] + s1r[j, i, :SIXTH].astype(f32)
        start(copies(S2, g, j))

    def stage3(g, j):
        arrive(copies(S2, g, j))
        sent(S1, g, j)
        for i in range(2):
            fin[j, i] = (acc[j, pl.ds(i * H, SIXTH)] + s2r[j, i].astype(f32)).astype(bf16)
        start(copies(G1, g, j))
        start(own(g, j))

    def stage4(g, j):
        for c in own(g, j):
            c.wait()
        arrive(copies(G1, g, j))
        sent(S2, g, j)
        start(copies(G2, g, j))

    def stage5(g, j):
        arrive(copies(G2, g, j))
        sent(G1, g, j)
        start(copies(G3, g, j))

    def stage6(g, j):
        arrive(copies(G3, g, j))
        sent(G2, g, j)
        sent(G3, g, j)

    def service(g, j, second):
        for fn, off in zip((stage1, stage2, stage3, stage4, stage5, stage6), OFFSETS):
            groups = GROUPS if fn in (stage1, stage2) else GROUPS - 1
            for back in range(3):
                shift = back * PERIOD - off - (0 if second else TILES)
                if -TILES < shift < TILES and (second or back > 0):
                    now = (g >= back) & (g - back < groups)
                    if shift < 0:
                        now = now & (j + shift >= 0)
                    if shift > 0:
                        now = now & (j + shift < TILES)

                    @pl.when(now)
                    def _():
                        fn(g - back, j + shift)

    start(x_copies(0))
    start(w_copies(0, 0))
    wd_copy(0, 0).start()

    barrier = pltpu.get_barrier_semaphore()
    for n in (pn, xn, yn):
        pl.semaphore_signal(barrier, inc=1, device_id={"tp": n}, device_id_type=MESH)
    pl.semaphore_wait(barrier, 3)

    def group(g, _):
        for c in x_copies(g):
            c.wait()

        def first(j, _):
            n = g * TILES + j
            slot = n % 2

            @pl.when(n + 1 < GROUPS * TILES)
            def _():
                start(w_copies(jnp.where(j + 1 < TILES, j + 1, 0), 1 - slot))

            service(g, j, False)
            for c in w_copies(j, slot):
                c.wait()
            r = jnp.dot(xbuf[...], whole[wrows(slot), :], preferred_element_type=f32)
            hid[:, pl.ds(pl.multiple_of(j * T1, T1), T1)] = (gelu(r[:, :T1]) * r[:, T1:]).astype(bf16)
            return 0

        lax.fori_loop(0, TILES, first, 0)

        @pl.when(g + 1 < GROUPS)
        def _():
            start(x_copies(g + 1))

        def second(j, _):
            n = g * TILES + j
            slot = n % 2

            @pl.when(n + 1 < GROUPS * TILES)
            def _():
                wd_copy(jnp.where(j + 1 < TILES, j + 1, 0), 1 - slot).start()

            service(g, j, True)
            wd_copy(j, slot).wait()
            r = jnp.dot(hid[...], wdbuf[slot], preferred_element_type=f32)
            acc[j] = r[:HALF]
            whole[srows(j), :] = r[HALF:].astype(bf16)
            start(copies(S0, g, j))
            return 0

        lax.fori_loop(0, TILES, second, 0)
        return 0

    lax.fori_loop(0, GROUPS, group, 0)

    def settle(j, first, rows, sem):
        at = pl.ds(pl.multiple_of(j * ROWS + first, GROUP), rows)
        return pltpu.make_async_copy(y.at[pl.ds(first, rows), columns(j)], whole.at[at], vsem.at[sem, j])

    def each(fn, first=0, end=TILES):
        def step(j, _):
            fn(j)
            return 0

        lax.fori_loop(first, end, step, 0)

    last, full, g = ROWS - GROUP, 2 * D // ROWS, GROUPS - 1
    each(lambda j: stage6(g - 1, j), min(TILES, 3 * TILES - OFFSETS[5]))
    each(lambda j: settle(j, 0, last, 0).start(), 0, full)
    each(lambda j: stage1(g, j), TILES - OFFSETS[0])
    each(lambda j: stage2(g, j), TILES - OFFSETS[1])
    each(lambda j: settle(j, 0, last, 0).start(), full)
    each(lambda j: stage3(g, j))
    each(lambda j: stage4(g, j))
    each(lambda j: stage5(g, j))

    def finish(j):
        stage6(g, j)
        settle(j, last, GROUP, 1).start()

    each(finish)
    for j in range(TILES):
        settle(j, 0, last, 0).wait()
        settle(j, last, GROUP, 1).wait()


def copy_kernel(whole, out, sem):
    rows = ROWS // PIECES
    cs = [
        pltpu.make_async_copy(whole.at[pl.ds(j * ROWS + i * rows, rows)], out.at[pl.ds(i * rows, rows), pl.ds(j * T2, T2)], sem.at[j, i])
        for i in range(PIECES)
        for j in range(TILES)
    ]
    for c in cs:
        c.start()
    for c in cs:
        c.wait()


def solution(mesh):
    bf16, f32 = jnp.bfloat16, jnp.float32

    def step(x, w_gate, w_up, w_down):
        _, whole = pl.pallas_call(
            kernel,
            out_shape=(jax.ShapeDtypeStruct((ROWS, D), bf16), pltpu.VMEM((TILES * ROWS, T2), bf16)),
            in_specs=[pl.BlockSpec(memory_space=pl.ANY)] * 4,
            out_specs=(pl.BlockSpec(memory_space=pl.ANY), pl.BlockSpec(memory_space=pltpu.VMEM)),
            scratch_shapes=[
                pltpu.VMEM((GROUP, D), bf16),
                pltpu.VMEM((2, FF, T2), bf16),
                pltpu.VMEM((GROUP, FF), bf16),
                pltpu.VMEM((TILES, HALF, T2), f32),
                pltpu.VMEM((TILES, 2, QUARTER, T2), bf16),
                pltpu.VMEM((TILES, 2, QUARTER, T2), bf16),
                pltpu.VMEM((TILES, 2, SIXTH, T2), bf16),
                pltpu.VMEM((TILES, 2, SIXTH, T2), bf16),
                pltpu.VMEM((TILES, 2, SIXTH, T2), bf16),
                pltpu.SemaphoreType.DMA((16,)),
                pltpu.SemaphoreType.DMA((2, 2)),
                pltpu.SemaphoreType.DMA((2,)),
                pltpu.SemaphoreType.DMA((10, TILES)),
                pltpu.SemaphoreType.DMA((10, TILES)),
                pltpu.SemaphoreType.DMA((2, TILES)),
                pltpu.SemaphoreType.DMA((2, TILES)),
            ],
            compiler_params=pltpu.CompilerParams(collective_id=0, has_side_effects=True, vmem_limit_bytes=42 * 2**20),
            cost_estimate=pl.CostEstimate(flops=6 * ROWS * D * FF, bytes_accessed=400 * 2**20, transcendentals=ROWS * FF),
        )(x, w_gate, w_up, w_down)
        return pl.pallas_call(
            copy_kernel,
            out_shape=jax.ShapeDtypeStruct((ROWS, D), bf16),
            in_specs=[pl.BlockSpec(memory_space=pltpu.VMEM)],
            out_specs=pl.BlockSpec(memory_space=pl.ANY),
            scratch_shapes=[pltpu.SemaphoreType.DMA((TILES, PIECES))],
            compiler_params=pltpu.CompilerParams(vmem_limit_bytes=4 * 2**20),
            cost_estimate=pl.CostEstimate(flops=0, bytes_accessed=2 * ROWS * D, transcendentals=0),
        )(whole)

    return jax.shard_map(
        step,
        mesh=mesh,
        in_specs=(P("dp", None), P(None, "tp"), P(None, "tp"), P("tp", None)),
        out_specs=P("dp", None),
        check_vma=False,
    )
```

```python
import math

import jax
import jax.numpy as jnp
from jax import lax
from jax.experimental import pallas as pl
from jax.experimental.pallas import tpu as pltpu
from jax.sharding import PartitionSpec as P

MESH = pl.DeviceIdType.MESH
ROWS, D, FF = 2048, 5376, 2688
GROUP = 512
HALF, QUARTER, SIXTH = GROUP // 2, GROUP // 8, GROUP // 16
GROUPS = ROWS // GROUP
T1 = 384
T2 = 768
TILES = FF // T1
PERIOD = 2 * TILES
OFFSETS = (2, 4, 7, 9, 12, 14)
PIECES = 4
S0, S1, S2, G1, G2, G3 = range(6)


def gelu(v):
    c = (2 / math.pi) ** 0.5
    return v * (0.5 + 0.5 * jnp.tanh(v * (c + (c * 0.044715) * (v * v))))


def kernel(x_hbm, wg, wu, wd, y, whole, xbuf, wdbuf, hid, acc, s1s, s1r, s2s, s2r, fin, xsem, wsem, wdsem, ssem, rsem, lsem, vsem):
    def wrows(slot):
        return pl.ds(pl.multiple_of(slot * D, 128), D)

    def srows(j, first=0, rows=HALF):
        return pl.ds(pl.multiple_of(2 * D + j * HALF + first, QUARTER), rows)

    def rrows(j, first=0, rows=HALF):
        return pl.ds(pl.multiple_of(2 * D + TILES * HALF + j * HALF + first, QUARTER), rows)

    me = lax.axis_index("tp")
    cx, cy, core = me // 4, (me // 2) % 2, me % 2
    pn = me + 1 - 2 * core
    xn = me + 4 - 8 * cx
    yn = me + 2 - 4 * cy

    a = lambda i, j: i * QUARTER + j * SIXTH
    b = lambda j, i: HALF // 2 + j * QUARTER + i * SIXTH
    blocks = (a(cx, cy), a(cx, 1 - cy), a(1 - cx, cy), a(1 - cx, 1 - cy), b(cy, cx), b(cy, 1 - cx), b(1 - cy, cx), b(1 - cy, 1 - cx))

    def x_copies(g):
        out = []
        for h, c in enumerate((core, 1 - core)):
            for k, off in enumerate(blocks):
                row = pl.multiple_of(g * GROUP + c * HALF + off, SIXTH)
                i = h * len(blocks) + k
                out.append(pltpu.make_async_copy(x_hbm.at[pl.ds(row, SIXTH)], xbuf.at[pl.ds(i * SIXTH, SIXTH)], xsem.at[i]))
        return out

    def w_copies(j, slot):
        cols = pl.ds(pl.multiple_of(j * T1, T1), T1)
        return [
            pltpu.make_async_copy(wg.at[:, cols], whole.at[wrows(slot), pl.ds(0, T1)], wsem.at[slot, 0]),
            pltpu.make_async_copy(wu.at[:, cols], whole.at[wrows(slot), pl.ds(T1, T1)], wsem.at[slot, 1]),
        ]

    def columns(j):
        return pl.ds(pl.multiple_of(j * T2, T2), T2)

    def wd_copy(j, slot):
        return pltpu.make_async_copy(wd.at[:, columns(j)], wdbuf.at[slot], wdsem.at[slot])

    def remote(src, dst, sem, j, to):
        return pltpu.make_async_remote_copy(src_ref=src, dst_ref=dst, send_sem=ssem.at[sem, j], recv_sem=rsem.at[sem, j], device_id={"tp": to}, device_id_type=MESH)

    def part(g, off, rows, j):
        return y.at[pl.ds(pl.multiple_of(g * GROUP + core * HALF + off, SIXTH), rows), columns(j)]

    def copies(stage, g, j):
        if stage == S0:
            return [remote(whole.at[srows(j)], whole.at[rrows(j)], S0, j, pn)]
        if stage == S1:
            return [remote(s1s.at[j, i], s1r.at[j, i], S1, j, (xn, yn)[i]) for i in range(2)]
        if stage == S2:
            return [remote(s2s.at[j, i], s2r.at[j, i], S2, j, (yn, xn)[i]) for i in range(2)]
        if stage == G1:
            return [remote(fin.at[j, i], part(g, blocks[4 * i], SIXTH, j), G1, j, (yn, xn)[i]) for i in range(2)]
        if stage == G2:
            offs = (cx * QUARTER, HALF // 2 + cy * QUARTER)
            return [remote(part(g, offs[i], QUARTER, j), part(g, offs[i], QUARTER, j), G2, j, (xn, yn)[i]) for i in range(2)]
        return [remote(part(g, 0, HALF, j), part(g, 0, HALF, j), G3, j, pn)]

    def own(g, j):
        return [pltpu.make_async_copy(fin.at[j, i], part(g, blocks[4 * i], SIXTH, j), lsem.at[i, j]) for i in range(2)]

    def start(cs):
        for c in cs:
            c.start()

    def both(stage, g, j):
        if stage in (S1, G2):
            return remote(s1s.at[j], s1r.at[j], stage, j, pn)
        if stage in (S2, G1):
            return remote(s2s.at[j], s2r.at[j], stage, j, pn)
        return copies(stage, g, j)[0]

    def arrive(stage, g, j):
        both(stage, g, j).wait_recv()

    f32, bf16 = jnp.float32, jnp.bfloat16
    Q, H = QUARTER, HALF // 2

    def sent(stage, g, j):
        both(stage, g, j).wait_send()

    def stage1(g, j):
        arrive(S0, g, j)
        for i in range(2):
            keep, send = pl.ds(i * H, Q), pl.ds(i * H + Q, Q)
            s1s[j, i] = (acc[j, send] + whole[rrows(j, i * H + Q, Q), :].astype(f32)).astype(bf16)
            acc[j, keep] = acc[j, keep] + whole[rrows(j, i * H, Q), :].astype(f32)
        start(copies(S1, g, j))

    def stage2(g, j):
        arrive(S1, g, j)
        sent(S0, g, j)
        for i in range(2):
            keep, send = pl.ds(i * H, SIXTH), pl.ds(i * H + SIXTH, SIXTH)
            s2s[j, i] = (acc[j, send] + s1r[j, i, SIXTH:].astype(f32)).astype(bf16)
            acc[j, keep] = acc[j, keep] + s1r[j, i, :SIXTH].astype(f32)
        start(copies(S2, g, j))

    def stage3(g, j):
        arrive(S2, g, j)
        sent(S1, g, j)
        for i in range(2):
            fin[j, i] = (acc[j, pl.ds(i * H, SIXTH)] + s2r[j, i].astype(f32)).astype(bf16)
        start(copies(G1, g, j))
        start(own(g, j))

    def stage4(g, j):
        for c in own(g, j):
            c.wait()
        arrive(G1, g, j)
        sent(S2, g, j)
        start(copies(G2, g, j))

    def stage5(g, j):
        arrive(G2, g, j)
        sent(G1, g, j)
        start(copies(G3, g, j))

    def stage6(g, j):
        arrive(G3, g, j)
        sent(G2, g, j)
        sent(G3, g, j)

    def service(g, j, second):
        for fn, off in zip((stage1, stage2, stage3, stage4, stage5, stage6), OFFSETS):
            groups = GROUPS if fn in (stage1, stage2) else GROUPS - 1
            for back in range(3):
                shift = back * PERIOD - off - (0 if second else TILES)
                if -TILES < shift < TILES and (second or back > 0):
                    now = (g >= back) & (g - back < groups)
                    if shift < 0:
                        now = now & (j + shift >= 0)
                    if shift > 0:
                        now = now & (j + shift < TILES)

                    @pl.when(now)
                    def _():
                        fn(g - back, j + shift)

    start(x_copies(0))
    start(w_copies(0, 0))
    wd_copy(0, 0).start()

    barrier = pltpu.get_barrier_semaphore()
    for n in (pn, xn, yn):
        pl.semaphore_signal(barrier, inc=1, device_id={"tp": n}, device_id_type=MESH)
    pl.semaphore_wait(barrier, 3)

    def group(g, _):
        for c in x_copies(g):
            c.wait()

        def first(j, _):
            n = g * TILES + j
            slot = n % 2

            @pl.when(n + 1 < GROUPS * TILES)
            def _():
                start(w_copies(jnp.where(j + 1 < TILES, j + 1, 0), 1 - slot))

            service(g, j, False)
            for c in w_copies(j, slot):
                c.wait()
            r = jnp.dot(xbuf[...], whole[wrows(slot), :], preferred_element_type=f32)
            hid[:, pl.ds(pl.multiple_of(j * T1, T1), T1)] = (gelu(r[:, :T1]) * r[:, T1:]).astype(bf16)
            return 0

        lax.fori_loop(0, TILES, first, 0)

        @pl.when(g + 1 < GROUPS)
        def _():
            start(x_copies(g + 1))

        def second(j, _):
            n = g * TILES + j
            slot = n % 2

            @pl.when(n + 1 < GROUPS * TILES)
            def _():
                wd_copy(jnp.where(j + 1 < TILES, j + 1, 0), 1 - slot).start()

            service(g, j, True)
            wd_copy(j, slot).wait()
            r = jnp.dot(hid[...], wdbuf[slot], preferred_element_type=f32)
            acc[j] = r[:HALF]
            whole[srows(j), :] = r[HALF:].astype(bf16)
            start(copies(S0, g, j))
            return 0

        lax.fori_loop(0, TILES, second, 0)
        return 0

    lax.fori_loop(0, GROUPS, group, 0)

    def settle(j, first, rows, sem):
        at = pl.ds(pl.multiple_of(j * ROWS + first, GROUP), rows)
        return pltpu.make_async_copy(y.at[pl.ds(first, rows), columns(j)], whole.at[at], vsem.at[sem, j])

    def each(fn, first=0, end=TILES):
        def step(j, _):
            fn(j)
            return 0

        lax.fori_loop(first, end, step, 0)

    last, full, g = ROWS - GROUP, 2 * D // ROWS, GROUPS - 1
    each(lambda j: stage6(g - 1, j), min(TILES, 3 * TILES - OFFSETS[5]))
    each(lambda j: settle(j, 0, last, 0).start(), 0, full)
    each(lambda j: stage1(g, j), TILES - OFFSETS[0])
    each(lambda j: stage2(g, j), TILES - OFFSETS[1])
    each(lambda j: settle(j, 0, last, 0).start(), full)
    each(lambda j: stage3(g, j))
    each(lambda j: stage4(g, j))
    each(lambda j: stage5(g, j))

    def finish(j):
        stage6(g, j)
        settle(j, last, GROUP, 1).start()

    each(finish)
    for j in range(TILES):
        settle(j, 0, last, 0).wait()
        settle(j, last, GROUP, 1).wait()


def copy_kernel(whole, out, sem):
    rows = ROWS // PIECES
    cs = [
        pltpu.make_async_copy(whole.at[pl.ds(j * ROWS + i * rows, rows)], out.at[pl.ds(i * rows, rows), pl.ds(j * T2, T2)], sem.at[j, i])
        for i in range(PIECES)
        for j in range(TILES)
    ]
    for c in cs:
        c.start()
    for c in cs:
        c.wait()


def solution(mesh):
    bf16, f32 = jnp.bfloat16, jnp.float32

    def step(x, w_gate, w_up, w_down):
        _, whole = pl.pallas_call(
            kernel,
            out_shape=(jax.ShapeDtypeStruct((ROWS, D), bf16), pltpu.VMEM((TILES * ROWS, T2), bf16)),
            in_specs=[pl.BlockSpec(memory_space=pl.ANY)] * 4,
            out_specs=(pl.BlockSpec(memory_space=pl.ANY), pl.BlockSpec(memory_space=pltpu.VMEM)),
            scratch_shapes=[
                pltpu.VMEM((GROUP, D), bf16),
                pltpu.VMEM((2, FF, T2), bf16),
                pltpu.VMEM((GROUP, FF), bf16),
                pltpu.VMEM((TILES, HALF, T2), f32),
                pltpu.VMEM((TILES, 2, QUARTER, T2), bf16),
                pltpu.VMEM((TILES, 2, QUARTER, T2), bf16),
                pltpu.VMEM((TILES, 2, SIXTH, T2), bf16),
                pltpu.VMEM((TILES, 2, SIXTH, T2), bf16),
                pltpu.VMEM((TILES, 2, SIXTH, T2), bf16),
                pltpu.SemaphoreType.DMA((16,)),
                pltpu.SemaphoreType.DMA((2, 2)),
                pltpu.SemaphoreType.DMA((2,)),
                pltpu.SemaphoreType.DMA((6, TILES)),
                pltpu.SemaphoreType.DMA((6, TILES)),
                pltpu.SemaphoreType.DMA((2, TILES)),
                pltpu.SemaphoreType.DMA((2, TILES)),
            ],
            compiler_params=pltpu.CompilerParams(collective_id=0, has_side_effects=True, vmem_limit_bytes=42 * 2**20),
            cost_estimate=pl.CostEstimate(flops=6 * ROWS * D * FF, bytes_accessed=400 * 2**20, transcendentals=ROWS * FF),
        )(x, w_gate, w_up, w_down)
        return pl.pallas_call(
            copy_kernel,
            out_shape=jax.ShapeDtypeStruct((ROWS, D), bf16),
            in_specs=[pl.BlockSpec(memory_space=pltpu.VMEM)],
            out_specs=pl.BlockSpec(memory_space=pl.ANY),
            scratch_shapes=[pltpu.SemaphoreType.DMA((TILES, PIECES))],
            compiler_params=pltpu.CompilerParams(vmem_limit_bytes=4 * 2**20),
            cost_estimate=pl.CostEstimate(flops=0, bytes_accessed=2 * ROWS * D, transcendentals=0),
        )(whole)

    return jax.shard_map(
        step,
        mesh=mesh,
        in_specs=(P("dp", None), P(None, "tp"), P(None, "tp"), P("tp", None)),
        out_specs=P("dp", None),
        check_vma=False,
    )
```
